32 devices in a mesh: seq: 8 (over y, x, core), grp: 4 (over z).
Axes of the slice: x: 2, y: 2, z: 4, core: 2. Of those that a mesh axis runs over, the one named last changes fastest.
Arguments:
- byte_ids: int32 [1536, 8], P('seq'), may hold values from 0 to 255
- patch_order: int32 [1536], P('seq'), may hold values from 0 to 1535, as said below
- query_rows: bfloat16 [1536, 8192], P('seq', 'grp'), may hold values from -25 to 25
- key_rows: bfloat16 [1536, 8192], P('seq', 'grp'), may hold values from -25 to 25
- value_rows: bfloat16 [1536, 8192], P('seq', 'grp'), may hold values from -6 to 6
- byte_embed: bfloat16 [256, 1024], replicated, may hold values from -6.5 to 6.5
- norm_gain: float32 [1024], replicated, may hold values from 0.25 to 1.75
- w_up: bfloat16 [1024, 4096], replicated, may hold values from -0.1875 to 0.1875
- w_down: bfloat16 [4096, 1024], replicated, may hold values from -0.09375 to 0.09375
- vocab_head: bfloat16 [1024, 256], replicated, may hold values from -12 to 12
Outputs:
- byte_loss: float32 [1536, 8], P(('seq', 'grp'))
- query_grad: bfloat16 [1536, 8192], P('seq', 'grp')
- key_grad: bfloat16 [1536, 8192], P('seq', 'grp')
- value_grad: bfloat16 [1536, 8192], P('seq', 'grp')
The draws below stay inside these ranges and needn't reach their ends.
Inputs may be any that keep to these rules, and one draw needn't show every extreme that they name: `patch_order`: each aligned block of 192 entries is a permutation of that block's own indices.
All inputs are finite; a program needn't handle non-finite values.
Results may differ from the reference program's by a relative error of at most 0.028.
Values may be sent and summed in bfloat16 or wider, within the bound.
A program may use at most 192 MiB of HBM per device.

```python
import math
import jax
import jax.numpy as jnp
from jax import lax

DG = 8192
DL = 1024
FFL = 4096
VOCAB = 256
HEAD = 128
PATCH = 8
P_DEV = 192
PATCHES = 1536


def drawn_rows(key, which):
    base = jnp.clip(jax.random.normal(jax.random.fold_in(key, 101 + which), (PATCHES, DG), jnp.float32), -4.0, 4.0)
    return (1.7 * base).astype(jnp.bfloat16)


def draw_query_rows(key, part):
    return drawn_rows(key, 0)


def draw_key_rows(key, part):
    return drawn_rows(key, 1)


def draw_patch_order(key, part):
    block_count = PATCHES // P_DEV
    keys = jax.random.split(jax.random.fold_in(key, 31), block_count)
    orders = jax.vmap(lambda single: jax.random.permutation(single, P_DEV))(keys)
    offsets = (jnp.arange(block_count, dtype=jnp.int32) * P_DEV)[:, None]
    return (orders.astype(jnp.int32) + offsets).reshape(PATCHES).astype(jnp.int32)


def draw_byte_embed(key, part):
    entries = jnp.clip(jax.random.normal(jax.random.fold_in(key, 301), (VOCAB, DL), jnp.float32), -4.0, 4.0)
    factor = jnp.exp(jax.random.uniform(jax.random.fold_in(key, 303), (VOCAB, 1), jnp.float32, 0.0, math.log(10.0)))
    return (0.1 * factor * entries).astype(jnp.bfloat16)


def draw_vocab_head(key, part):
    entries = jnp.clip(jax.random.normal(jax.random.fold_in(key, 401), (DL, VOCAB), jnp.float32), -4.0, 4.0) * (3.0 / math.sqrt(DL))
    return jnp.clip(entries, -11.5, 11.5).astype(jnp.bfloat16)


def place_ends(array, key, smallest, top_value):
    longest = array.shape.index(max(array.shape))
    spots = []
    for shift in (0, 1):
        where = [jax.random.randint(jax.random.fold_in(key, axis), (), 0, length) for axis, length in enumerate(array.shape)]
        where[longest] = (where[longest] + shift) % array.shape[longest]
        spots.append(tuple(where))
    return array.at[spots[0]].set(smallest).at[spots[1]].set(top_value)


def level_of(key, extent, shards, smallest, top_value):
    level = 1.0
    for axis_at, blocks in shards:
        draws = jax.random.uniform(jax.random.fold_in(jax.random.fold_in(key, 6), axis_at), (blocks,), jnp.float32, smallest / len(shards), top_value / len(shards))
        level = level * jnp.repeat(jnp.exp(draws), extent[axis_at] // blocks).reshape((-1,) + (1,) * (len(extent) - 1 - axis_at))
    return level


def centred(own_key, dims, scale, reach, pieces=(), kind=jnp.bfloat16):
    values = jax.random.normal(own_key, dims, jnp.float32) * scale
    if len(pieces) > 0:
        values = level_of(own_key, dims, pieces, -0.22, 0.18) * values
    return jnp.clip(values, min=-reach, max=reach).astype(kind)


def setup_inputs(seed: int = 0) -> dict:
    splits = jax.random.split(jax.random.key(seed), 11)
    byte_ids = place_ends(jax.random.randint(splits[0], (PATCHES, PATCH), 0, VOCAB), jax.random.fold_in(splits[0], 1), 0, VOCAB - 1).astype(jnp.int32)
    patch_order = draw_patch_order(jax.random.fold_in(splits[10], 71), 0)
    query_rows = draw_query_rows(jax.random.fold_in(splits[10], 71), 0)
    key_rows = draw_key_rows(jax.random.fold_in(splits[10], 71), 0)
    value_rows = centred(splits[4], (PATCHES, DG), 1.0, 6.0, ((0, 8), (1, 4)))
    byte_embed = draw_byte_embed(jax.random.fold_in(splits[10], 71), 0)
    norm_gain = jnp.clip(1.0 + 0.15 * jax.random.normal(splits[6], (DL,), jnp.float32), 0.25, 1.75)
    w_up = centred(splits[7], (DL, FFL), DL ** -0.5, 0.1875)
    w_down = centred(splits[8], (FFL, DL), FFL ** -0.5, 0.09375)
    vocab_head = draw_vocab_head(jax.random.fold_in(splits[10], 71), 0)
    return dict(byte_ids=byte_ids, patch_order=patch_order, query_rows=query_rows, key_rows=key_rows, value_rows=value_rows, byte_embed=byte_embed, norm_gain=norm_gain, w_up=w_up, w_down=w_down, vocab_head=vocab_head)


EPSILON = 1e-05

def local_model(context, byte_ids, byte_embed, norm_gain, w_up, w_down, vocab_head):
    patch_count = context.shape[0]
    model_width = byte_embed.shape[1]
    vocab_size = vocab_head.shape[1]
    hidden_in = context.astype(jnp.float32).reshape(patch_count * PATCH, model_width)
    previous = jnp.concatenate([byte_ids[:, :1], byte_ids[:, :-1]], axis=1).reshape(-1)
    live_rows = jnp.tile(jnp.arange(PATCH) > 0, patch_count)
    letters = jnp.arange(vocab_size)
    one_hot = ((previous[:, None] == letters[None, :]) & live_rows[:, None]).astype(jnp.bfloat16)
    hidden_in = hidden_in + jnp.dot(one_hot, byte_embed, preferred_element_type=jnp.float32)
    inverse_rms = lax.rsqrt(lax.optimization_barrier(jnp.mean(hidden_in * hidden_in, axis=1, keepdims=True)) + EPSILON)
    normed = (hidden_in * inverse_rms * norm_gain).astype(jnp.bfloat16)
    raised = jnp.dot(normed, w_up, preferred_element_type=jnp.float32)
    active = jax.nn.gelu(raised, approximate=True).astype(jnp.bfloat16)
    after_mlp = hidden_in + jnp.dot(active, w_down, preferred_element_type=jnp.float32)
    final_scale = lax.rsqrt(lax.optimization_barrier(jnp.mean(after_mlp * after_mlp, axis=1, keepdims=True)) + EPSILON)
    final_rows = (after_mlp * final_scale).astype(jnp.bfloat16)
    logits = jnp.dot(final_rows, vocab_head, preferred_element_type=jnp.float32)
    row_top = lax.stop_gradient(lax.optimization_barrier(jnp.max(logits, axis=1, keepdims=True)))
    log_total = jnp.log(lax.optimization_barrier(jnp.sum(jnp.exp(logits - row_top), axis=1))) + row_top[:, 0]
    target = byte_ids.reshape(-1)
    chosen = lax.optimization_barrier(jnp.sum(jnp.where(target[:, None] == letters[None, :], logits, 0.0), axis=1))
    return (log_total - chosen).reshape(patch_count, PATCH)

def visible(size):
    order = jnp.arange(size)
    return order[None, :] <= order[:, None]

def head_scores(queries, key_side):
    return jnp.dot(queries, key_side.T, preferred_element_type=jnp.float32) * HEAD ** (-0.5)

def head_forward(operands):
    queries, key_side, value_side = operands
    scores = head_scores(queries, key_side)
    allowed = visible(scores.shape[0])
    row_top = lax.optimization_barrier(jnp.max(jnp.where(allowed, scores, -1e+30), axis=1, keepdims=True))
    spread = jnp.where(allowed, jnp.exp(jnp.where(allowed, scores - row_top, -1e+30)), 0.0)
    log_mass = row_top[:, 0] + jnp.log(lax.optimization_barrier(jnp.sum(spread, axis=1)))
    shifted = jnp.where(allowed, scores - log_mass[:, None], -1e+30)
    weights = jnp.where(allowed, jnp.exp(shifted), 0.0)
    attended = jnp.dot(weights, value_side.astype(jnp.float32), precision=lax.Precision.HIGHEST).astype(jnp.bfloat16)
    return (attended, log_mass)

def head_backward(operands):
    queries, key_side, value_side, attended, log_mass, out_grad = operands
    scores = head_scores(queries, key_side)
    allowed = visible(scores.shape[0])
    shifted = jnp.where(allowed, scores - log_mass[:, None], -1e+30)
    chances = jnp.where(allowed, jnp.exp(shifted), 0.0)
    row_dot = lax.optimization_barrier(jnp.sum(out_grad.astype(jnp.float32) * attended.astype(jnp.float32), axis=1))
    chance_grad = jnp.dot(out_grad, value_side.T, preferred_element_type=jnp.float32)
    score_grad = (chances * (chance_grad - row_dot[:, None])).astype(jnp.bfloat16)
    query_grad = (jnp.dot(score_grad, key_side, preferred_element_type=jnp.float32) * HEAD ** (-0.5)).astype(jnp.bfloat16)
    key_grad = (jnp.dot(score_grad.T, queries, preferred_element_type=jnp.float32) * HEAD ** (-0.5)).astype(jnp.bfloat16)
    value_grad = jnp.dot(chances.astype(jnp.bfloat16).T, out_grad, preferred_element_type=jnp.float32).astype(jnp.bfloat16)
    return (query_grad, key_grad, value_grad)

def by_heads(matrix):
    return matrix.reshape(matrix.shape[0], -1, HEAD).transpose(1, 0, 2)

def from_heads(stack):
    return stack.transpose(1, 0, 2).reshape(stack.shape[1], -1)

def reference(byte_ids, patch_order, query_rows, key_rows, value_rows, byte_embed, norm_gain, w_up, w_down, vocab_head):
    split_query = by_heads(query_rows)
    split_key = by_heads(key_rows)
    split_value = by_heads(value_rows)
    attended_stack, log_mass = lax.map(head_forward, (split_query, split_key, split_value))
    attended = from_heads(attended_stack)

    def scored(context):
        return local_model(context, byte_ids, byte_embed, norm_gain, w_up, w_down, vocab_head)
    byte_loss, pull_back = jax.vjp(scored, attended)
    context_grad, = pull_back(jnp.ones_like(byte_loss))
    grads = lax.map(head_backward, (split_query, split_key, split_value, attended_stack, log_mass, by_heads(context_grad)))
    return (byte_loss[patch_order], from_heads(grads[0]), from_heads(grads[1]), from_heads(grads[2]))
```

```python
import functools

import jax
import jax.numpy as jnp
from jax import lax
from jax.experimental import pallas as pl
from jax.experimental.pallas import tpu as pltpu
from jax.sharding import PartitionSpec as P

HEAD = 128
PATCH = 8


EPSILON = 1e-05
FLOOR = -1e30


def shortened(value):
    return jax.tree.map(lambda a: a.astype(jnp.bfloat16) if a.dtype == jnp.float32 else a, value)


def partner_2(value, axis, bit):
    mask = 2**bit
    pairs = [(source, source ^ mask) for source in range(lax.axis_size(axis))]
    return lax.ppermute(value, axis, pairs)


def local_model(context, byte_ids, byte_embed, norm_gain, w_up, w_down, vocab_head):
    patch_count = context.shape[0]
    model_width = byte_embed.shape[1]
    vocab_size = vocab_head.shape[1]
    hidden_in = context.astype(jnp.float32).reshape(patch_count * PATCH, model_width)
    previous = jnp.concatenate([byte_ids[:, :1], byte_ids[:, :-1]], axis=1).reshape(-1)
    live_rows = jnp.tile(jnp.arange(PATCH) > 0, patch_count)
    letters = jnp.arange(vocab_size)
    one_hot = ((previous[:, None] == letters[None, :]) & live_rows[:, None]).astype(jnp.bfloat16)
    hidden_in = hidden_in + jnp.dot(one_hot, byte_embed, preferred_element_type=jnp.float32)
    inverse_rms = lax.rsqrt(jnp.mean(hidden_in * hidden_in, axis=1, keepdims=True) + EPSILON)
    normed = (hidden_in * inverse_rms * norm_gain).astype(jnp.bfloat16)
    raised = jnp.dot(normed, w_up, preferred_element_type=jnp.float32)
    active = jax.nn.gelu(raised, approximate=True).astype(jnp.bfloat16)
    after_mlp = hidden_in + jnp.dot(active, w_down, preferred_element_type=jnp.float32)
    final_scale = lax.rsqrt(jnp.mean(after_mlp * after_mlp, axis=1, keepdims=True) + EPSILON)
    final_rows = (after_mlp * final_scale).astype(jnp.bfloat16)
    logits = jnp.dot(final_rows, vocab_head, preferred_element_type=jnp.float32)
    row_top = lax.stop_gradient(jnp.max(logits, axis=1, keepdims=True))
    log_total = jnp.log(jnp.sum(jnp.exp(logits - row_top), axis=1)) + row_top[:, 0]
    target = byte_ids.reshape(-1)
    chosen = jnp.sum(jnp.where(target[:, None] == letters[None, :], logits, 0.0), axis=1)
    return (log_total - chosen).reshape(patch_count, PATCH)


def head_order(flat, head_count, segments, seq_count):
    row_total = flat.shape[0]
    block_rows = row_total // segments
    arranged = flat.reshape(block_rows, segments, head_count, HEAD).transpose(2, 1, 0, 3)
    return arranged.reshape(seq_count, -1, block_rows, HEAD)


def row_order(stack, head_count, segments):
    block_rows = stack.shape[2]
    arranged = stack.reshape(head_count, segments, block_rows, HEAD).transpose(2, 1, 0, 3)
    return arranged.reshape(block_rows * segments, head_count * HEAD)


def shards(
    byte_ids,
    patch_order,
    query_rows,
    key_rows,
    value_rows,
    byte_embed,
    norm_gain,
    w_up,
    w_down,
    vocab_head,
):
    row_count = query_rows.shape[0]
    head_count = query_rows.shape[1] // HEAD
    seq_here = lax.axis_index("seq")
    grp_here = lax.axis_index("grp")
    first_here = seq_here * row_count
    seq_count = lax.axis_size("seq")
    segments = max(1, seq_count // head_count)
    held_heads = max(1, head_count // seq_count)
    bit_count = segments.bit_length() - 1
    residue = seq_here % segments
    arranged = tuple(
        (
            head_order(member, head_count, segments, seq_count)
            for member in (query_rows, key_rows, value_rows)
        )
    )
    own_query, own_key, own_value = jax.tree.map(
        lambda part, own: part.astype(own.dtype),
        lax.all_to_all(shortened(arranged), "seq", split_axis=0, concat_axis=2, tiled=True),
        arranged,
    )
    stacked = jnp.stack([own_key, own_value])
    for bit in range(bit_count):
        partner = partner_2(shortened(stacked), "seq", bit).astype(stacked.dtype)
        upper_half = seq_here >> bit & 1 == 1
        stacked = jnp.where(
            upper_half,
            jnp.concatenate([partner, stacked], 1),
            jnp.concatenate([stacked, partner], 1),
        )
    slot_count = own_query.shape[2]
    full_pairs = stacked.transpose(0, 2, 3, 1, 4).reshape(
        2, held_heads, slot_count * segments, HEAD
    )
    full_key = full_pairs[0]
    full_value = full_pairs[1]
    head_queries = own_query[0]
    query_pos = jnp.arange(slot_count, dtype=jnp.int32) * segments + residue
    key_pos = jnp.arange(slot_count * segments, dtype=jnp.int32)
    allowed = (key_pos[None, :] <= query_pos[:, None])[None]
    scores = jnp.einsum(
        "hqd,hkd->hqk", head_queries, full_key, preferred_element_type=jnp.float32
    ) * HEAD ** (-0.5)
    row_top = jnp.max(jnp.where(allowed, scores, FLOOR), axis=2, keepdims=True)
    spread = jnp.where(allowed, jnp.exp(jnp.where(allowed, scores - row_top, FLOOR)), 0.0)
    head_mass = row_top[:, :, 0] + jnp.log(jnp.sum(spread, axis=2))
    chances = jnp.where(
        allowed, jnp.exp(jnp.where(allowed, scores - head_mass[:, :, None], FLOOR)), 0.0
    )
    rounded_weights = chances.astype(jnp.bfloat16)
    head_attended = jnp.einsum(
        "hqk,hkd->hqd", chances, full_value.astype(jnp.float32), precision=lax.Precision.HIGHEST
    ).astype(jnp.bfloat16)
    attended = row_order(
        lax.all_to_all(head_attended[None], "seq", split_axis=2, concat_axis=0, tiled=True),
        head_count,
        segments,
    )
    local_order = patch_order - first_here
    ordered = jnp.take(attended, local_order, axis=0)
    owned_rows = lax.all_to_all(ordered, "grp", split_axis=0, concat_axis=1, tiled=True)
    group_rows = owned_rows.shape[0]
    slot_patches = lax.dynamic_slice_in_dim(local_order, grp_here * group_rows, group_rows, 0)
    slot_bytes = jnp.take(byte_ids, slot_patches, axis=0)

    def scored(context):
        return local_model(context, slot_bytes, byte_embed, norm_gain, w_up, w_down, vocab_head)

    byte_loss, pull_back = jax.vjp(scored, owned_rows)
    (context_grad,) = pull_back(jnp.ones_like(byte_loss))
    returned = lax.all_to_all(context_grad, "grp", split_axis=1, concat_axis=0, tiled=True)
    grads_flat = jnp.zeros_like(returned).at[local_order].set(returned)
    arranged_grads = head_order(grads_flat, head_count, segments, seq_count)
    grad_heads = lax.all_to_all(arranged_grads, "seq", split_axis=0, concat_axis=2, tiled=True)[0]
    head_dot = jnp.sum(grad_heads.astype(jnp.float32) * head_attended.astype(jnp.float32), axis=2)
    chance_grad = jnp.einsum(
        "hqd,hkd->hqk", grad_heads, full_value, preferred_element_type=jnp.float32
    )
    score_grad = (chances * (chance_grad - head_dot[:, :, None])).astype(jnp.bfloat16)
    query_heads = (
        jnp.einsum("hqk,hkd->hqd", score_grad, full_key, preferred_element_type=jnp.float32)
        * HEAD ** (-0.5)
    ).astype(jnp.bfloat16)
    key_part = jnp.einsum(
        "hqk,hqd->hkd", score_grad, head_queries, preferred_element_type=jnp.float32
    ) * HEAD ** (-0.5)
    value_part = jnp.einsum(
        "hqk,hqd->hkd", rounded_weights, grad_heads, preferred_element_type=jnp.float32
    )
    partial_pairs = (
        jnp.stack([key_part, value_part])
        .reshape(2, held_heads, slot_count, segments, HEAD)
        .transpose(0, 3, 1, 2, 4)
    )
    for bit in reversed(range(bit_count)):
        half_count = partial_pairs.shape[1] // 2
        upper_half = seq_here >> bit & 1 == 1
        lower_part = partial_pairs[:, :half_count]
        upper_part = partial_pairs[:, half_count:]
        kept_half = jnp.where(upper_half, upper_part, lower_part)
        sent_half = jnp.where(upper_half, lower_part, upper_part)
        partial_pairs = kept_half + partner_2(sent_half.astype(jnp.bfloat16), "seq", bit).astype(
            sent_half.dtype
        )
    key_heads = partial_pairs[0].astype(jnp.bfloat16)
    value_heads = partial_pairs[1].astype(jnp.bfloat16)
    back_query, back_key, back_value = (
        lax.all_to_all(query_heads[None], "seq", split_axis=2, concat_axis=0, tiled=True),
        lax.all_to_all(key_heads, "seq", split_axis=2, concat_axis=0, tiled=True),
        lax.all_to_all(value_heads, "seq", split_axis=2, concat_axis=0, tiled=True),
    )
    query_out = row_order(back_query, head_count, segments)
    key_out = row_order(back_key, head_count, segments)
    value_out = row_order(back_value, head_count, segments)
    return (byte_loss, query_out, key_out, value_out)


MESH = pl.DeviceIdType.MESH
LANES = 128
KEY_TILE = 256
HIDDEN_TILE = 1024
GELU_A = 0.7978845608028654
GELU_B = 0.044715
LOG2E = 1.4426950408889634
SCALE = HEAD ** (-0.5)


def dot_nn(a, b):
    return lax.dot_general(a, b, (((1,), (0,)), ((), ())), preferred_element_type=jnp.float32)


def dot_nt(a, b):
    return lax.dot_general(a, b, (((1,), (1,)), ((), ())), preferred_element_type=jnp.float32)


def dot_tn(a, b):
    return lax.dot_general(a, b, (((0,), (0,)), ((), ())), preferred_element_type=jnp.float32)


def dot_exact(a, b, dims):
    return lax.dot_general(
        a, b, (dims, ((), ())), precision=lax.Precision.HIGHEST, preferred_element_type=jnp.float32
    )


def fused_kernel(
    seq_count,
    grp_count,
    ids_in,
    order_in,
    gain_in,
    q_in,
    k_in,
    v_in,
    embed_in,
    up_in,
    down_in,
    vocab_in,
    loss_out,
    dq_out,
    dk_out,
    dv_out,
    q_buf,
    k_buf,
    v_buf,
    p_buf,
    att,
    ctx,
    dctx,
    dout,
    dq_buf,
    dk_buf,
    dv_buf,
    q_turned,
    g_turned,
    embed,
    up,
    down,
    up_turned,
    down_turned,
    vocab,
    ids,
    order,
    gain,
    hid,
    normed,
    slope,
    acc,
    dafter,
    dafter_low,
    losses,
    in_recv,
    in_send,
    weight_sem,
    ctx_recv,
    ctx_send,
    grad_recv,
    grad_send,
    loss_recv,
    loss_send,
    out_recv,
    out_send,
):
    me_s = lax.axis_index("seq")
    me_g = lax.axis_index("grp")
    jobs, total, _ = q_buf.shape
    rows = total // seq_count
    part = rows // grp_count
    model = embed.shape[1]
    vocab_size = embed.shape[0]
    ffl = up.shape[1]

    barrier = pltpu.get_barrier_semaphore()

    def greet_seq(d, _):
        peer = lax.rem(me_s + d, seq_count)
        pl.semaphore_signal(barrier, inc=1, device_id=(peer, me_g), device_id_type=MESH)
        return 0

    def greet_grp(d, _):
        peer = lax.rem(me_g + d, grp_count)
        pl.semaphore_signal(barrier, inc=1, device_id=(me_s, peer), device_id_type=MESH)
        return 0

    lax.fori_loop(1, grp_count, greet_grp, 0)
    lax.fori_loop(1, seq_count, greet_seq, 0)

    weight_copies = [
        pltpu.make_async_copy(a, b, weight_sem.at[n])
        for n, (a, b) in enumerate(
            (
                (ids_in, ids),
                (embed_in, embed),
                (gain_in, gain),
                (vocab_in, vocab),
                (up_in, up),
                (down_in, down),
                (order_in, order),
            )
        )
    ]
    for copy in weight_copies:
        copy.start()

    def block_of(index, size):
        return pl.ds(pl.multiple_of(index * size, size), size)

    def out_cols(job, owner):
        return block_of(job * seq_count + owner, HEAD)

    my_rows = block_of(me_s, rows)
    my_head = block_of(me_s, HEAD)
    arrays = ((k_in, k_buf), (q_in, q_buf), (v_in, v_buf))
    for job in range(jobs):
        for n, (source, target) in enumerate(arrays):
            pltpu.make_async_copy(
                source.at[:, out_cols(job, me_s)], target.at[job, my_rows], in_recv.at[job, n]
            ).start()
    pl.semaphore_wait(barrier, seq_count - 1 + grp_count - 1)

    whole = pl.ds(0, rows)
    halves = (pl.ds(0, rows // 2), pl.ds(rows // 2, rows // 2))

    def send_in(job, n, piece=whole):
        source, target = arrays[n]
        there = pl.ds(pl.multiple_of(me_s * rows + piece.start, piece.size), piece.size)

        def send_one(d, _):
            peer = lax.rem(me_s + d, seq_count)
            pltpu.make_async_remote_copy(
                src_ref=source.at[piece, out_cols(job, peer)],
                dst_ref=target.at[job, there],
                send_sem=in_send.at[n],
                recv_sem=in_recv.at[job, n],
                device_id=(peer, me_g),
                device_id_type=MESH,
            ).start()
            return 0

        lax.fori_loop(1, seq_count, send_one, 0)

    def wait_in(job, n):
        target = arrays[n][1].at[job]
        pltpu.make_async_copy(target, target, in_recv.at[job, n]).wait()

    widths = [-(-((i + 1) * rows) // KEY_TILE) * KEY_TILE for i in range(seq_count)]

    def letters_hot(t):
        letters = lax.broadcasted_iota(jnp.int32, (vocab_size, rows), 0)
        return letters == ids[pl.ds(t, 1), :]

    def embed_bytes(job):
        byte = me_g * jobs + job
        hot = letters_hot(jnp.maximum(byte - 1, 0)) & (byte > 0)
        hid[job] = dot_tn(hot.astype(jnp.bfloat16), embed[...])

    def weigh(job):
        for i, w in enumerate(widths):
            start = i * rows // LANES * LANES
            s = dot_nt(q_buf[job, i * rows : (i + 1) * rows], k_buf[job, :w])
            tail = s[:, start:]
            key_pos = lax.broadcasted_iota(jnp.int32, tail.shape, 1) + start
            query_pos = lax.broadcasted_iota(jnp.int32, tail.shape, 0) + i * rows
            tail = jnp.where(key_pos <= query_pos, tail, FLOOR)
            if start:
                s = jnp.concatenate([s[:, :start], tail], axis=1)
            else:
                s = tail
            top = jnp.max(s, axis=1, keepdims=True)
            e = jnp.exp2((s - top) * (SCALE * LOG2E))
            inverse = 1.0 / jnp.sum(e, axis=1, keepdims=True)
            p_buf[job, i * rows : (i + 1) * rows, :w] = (e * inverse).astype(jnp.bfloat16)

    def turn(source, target):
        for c in range(total // KEY_TILE):
            here = slice(c * KEY_TILE, (c + 1) * KEY_TILE)
            target[:, here] = source[here, :].astype(jnp.float32).T.astype(jnp.bfloat16)

    def turn_weights():
        def turn_chunk(c, _):
            chunk = block_of(c, KEY_TILE)
            for k in range(model // KEY_TILE):
                here = slice(k * KEY_TILE, (k + 1) * KEY_TILE)
                up_turned[chunk, here] = up[here, chunk].T
                down_turned[here, chunk] = down[chunk, here].T
            return 0

        lax.fori_loop(0, ffl // KEY_TILE, turn_chunk, 0)

    def attend(job):
        def send_ctx(i):
            @pl.when(me_s != i)
            def _():
                pltpu.make_async_remote_copy(
                    src_ref=att.at[job, i * rows : (i + 1) * rows],
                    dst_ref=ctx.at[job, :, my_head],
                    send_sem=ctx_send,
                    recv_sem=ctx_recv.at[job],
                    device_id=(i, me_g),
                    device_id_type=MESH,
                ).start()

        for i, w in enumerate(widths):
            here = slice(i * rows, (i + 1) * rows)
            att[job, here] = dot_nn(p_buf[job, here, :w], v_buf[job, :w]).astype(jnp.bfloat16)
            if i:
                send_ctx(i - 1)
        ctx[job, :, my_head] = att[job, my_rows]
        send_ctx(seq_count - 1)

    def byte_model(job):
        others = ctx.at[job, :, : (seq_count - 1) * HEAD]
        pltpu.make_async_copy(others, others, ctx_recv.at[job]).wait()
        h0 = hid[job] + ctx[job].astype(jnp.float32)
        hid[job] = h0
        inverse_rms = lax.rsqrt(jnp.mean(h0 * h0, axis=1, keepdims=True) + EPSILON)
        normed[...] = (h0 * inverse_rms * gain[...]).astype(jnp.bfloat16)
        acc[...] = h0

        for c in range(ffl // HIDDEN_TILE):
            chunk = slice(c * HIDDEN_TILE, (c + 1) * HIDDEN_TILE)
            x = dot_nn(normed[...], up[:, chunk])
            square = x * x
            th = jnp.tanh(x * (GELU_A + (GELU_A * GELU_B) * square))
            half = 0.5 + 0.5 * th
            active = (x * half).astype(jnp.bfloat16)
            slope[:, chunk] = half + (0.5 * x) * (1.0 - th * th) * (
                GELU_A + (3.0 * GELU_A * GELU_B) * square
            )
            acc[...] += dot_nn(active, down[chunk, :])
        after = acc[...]
        final_scale = lax.rsqrt(jnp.mean(after * after, axis=1, keepdims=True) + EPSILON)
        final_rows = (after * final_scale).astype(jnp.bfloat16)
        logits = dot_nn(final_rows, vocab[...])
        top = jnp.max(logits, axis=1, keepdims=True)
        e = jnp.exp(logits - top)
        z = jnp.sum(e, axis=1, keepdims=True)
        byte = me_g * jobs + job
        same = lax.broadcasted_iota(jnp.int32, (vocab_size, vocab_size), 0)
        same = same == lax.broadcasted_iota(jnp.int32, (vocab_size, vocab_size), 1)
        hot = dot_tn(letters_hot(byte).astype(jnp.bfloat16), same.astype(jnp.bfloat16))
        loss = jnp.log(z) + top - jnp.sum(hot * logits, axis=1, keepdims=True)
        lane = lax.broadcasted_iota(jnp.int32, (rows, LANES), 1)
        before = losses[me_g] if job else jnp.zeros((rows, LANES), jnp.float32)
        losses[me_g] = jnp.where(lane == byte, loss, before)
        dlogits = (e / z - hot).astype(jnp.bfloat16)
        dfinal = dot_nt(dlogits, vocab[...]).astype(jnp.bfloat16).astype(jnp.float32)
        after = acc[...]
        share = jnp.mean(dfinal * after, axis=1, keepdims=True)
        da = final_scale * dfinal - after * (final_scale * final_scale * final_scale * share)
        dafter[...] = da
        dafter_low[...] = da.astype(jnp.bfloat16)
        acc[...] = jnp.zeros_like(acc)

        for c in range(ffl // HIDDEN_TILE):
            chunk = slice(c * HIDDEN_TILE, (c + 1) * HIDDEN_TILE)
            dactive = dot_nn(dafter_low[...], down_turned[:, chunk]).astype(jnp.bfloat16)
            draised = (dactive.astype(jnp.float32) * slope[:, chunk]).astype(jnp.bfloat16)
            acc[...] += dot_nn(draised, up_turned[chunk, :])
        dn = acc[...].astype(jnp.bfloat16).astype(jnp.float32) * gain[...]
        h0 = hid[job]
        share = jnp.mean(dn * h0, axis=1, keepdims=True)
        dh = inverse_rms * dn - h0 * (inverse_rms * inverse_rms * inverse_rms * share)
        dctx[job] = (dh + dafter[...]).astype(jnp.bfloat16)
        dout[job, my_rows] = dctx[job, :, my_head]

        def send_grad(d, _):
            peer = lax.rem(me_s + d, seq_count)
            pltpu.make_async_remote_copy(
                src_ref=dctx.at[job, :, block_of(peer, HEAD)],
                dst_ref=dout.at[job, my_rows],
                send_sem=grad_send,
                recv_sem=grad_recv.at[job],
                device_id=(peer, me_g),
                device_id_type=MESH,
            ).start()
            return 0

        lax.fori_loop(1, seq_count, send_grad, 0)

    def send_losses():
        def send_loss(d, _):
            pltpu.make_async_remote_copy(
                src_ref=losses.at[me_g],
                dst_ref=losses.at[me_g],
                send_sem=loss_send,
                recv_sem=loss_recv,
                device_id=(me_s, lax.rem(me_g + d, grp_count)),
                device_id_type=MESH,
            ).start()
            return 0

        lax.fori_loop(1, grp_count, send_loss, 0)

    def send_out(job, n, i, source, target, piece=whole):
        here = source.at[job, pl.ds(i * rows + piece.start, piece.size)]
        there = target.at[piece, out_cols(job, me_s)]

        @pl.when(me_s != i)
        def _():
            pltpu.make_async_remote_copy(
                src_ref=here,
                dst_ref=there,
                send_sem=out_send.at[n],
                recv_sem=out_recv.at[n],
                device_id=(i, me_g),
                device_id_type=MESH,
            ).start()

        @pl.when(me_s == i)
        def _():
            pltpu.make_async_copy(here, there, out_recv.at[n]).start()

    firsts = [
        next(i for i, w in enumerate(widths) if w >= (c + 1) * KEY_TILE) * rows
        for c in range(total // KEY_TILE)
    ]

    def clear_edges():
        for c, first in enumerate(firsts):
            if first % LANES:
                above = slice(first // LANES * LANES, first)
                here = slice(c * KEY_TILE, (c + 1) * KEY_TILE)
                p_buf[:, above, here] = jnp.zeros((jobs, first % LANES, KEY_TILE), jnp.bfloat16)

    def key_side(job, turned, matrix, result, factor):
        for c in range(total // KEY_TILE):
            first = firsts[c] // LANES * LANES
            here = slice(c * KEY_TILE, (c + 1) * KEY_TILE)
            block = dot_nn(turned[:, first:], matrix[first:, here])
            if factor is not None:
                block = block * factor
            result[job, here] = block.T.astype(jnp.bfloat16)

    def send_keys(job, piece):
        for i in range(seq_count):
            send_out(job, 1, i, dk_buf, dk_out, piece)

    def value_side(job):
        turn(dout.at[job], g_turned)
        key_side(job, g_turned, p_buf.at[job], dv_buf, None)
        for i in range(seq_count):
            send_out(job, 2, i, dv_buf, dv_out)

    def query_side(job, kept):
        for i, w in enumerate(widths):
            here = slice(i * rows, (i + 1) * rows)
            g = dout[job, here]
            row_dot = jnp.sum(
                g.astype(jnp.float32) * att[job, here].astype(jnp.float32), axis=1, keepdims=True
            )
            dp = dot_nt(g, v_buf[job, :w])
            ds = (p_buf[job, here, :w].astype(jnp.float32) * (dp - row_dot)).astype(jnp.bfloat16)
            kept[here, :w] = ds
            dq_buf[job, here] = (dot_nn(ds, k_buf[job, :w]) * SCALE).astype(jnp.bfloat16)
            if i:
                send_out(job, 0, i - 1, dq_buf, dq_out)
        send_out(job, 0, seq_count - 1, dq_buf, dq_out)

    def wait_grad(job):
        others = dout.at[job, : (seq_count - 1) * rows]
        pltpu.make_async_copy(others, others, grad_recv.at[job]).wait()

    def attend_back(job):
        wait_grad(job)
        value_side(job)
        query_side(job, p_buf.at[job])
        key_side(job, q_turned.at[job], p_buf.at[job], dk_buf, SCALE)
        send_keys(job, halves[0])

    def attend_back_last(job):
        wait_grad(job)
        query_side(job, p_buf.at[job - 1])
        value_side(job)
        key_side(job, q_turned.at[job], p_buf.at[job - 1], dk_buf, SCALE)
        send_keys(job, whole)

    def attend_fore(job):
        wait_in(job, 0)
        wait_in(job, 1)
        weigh(job)
        turn(q_buf.at[job], q_turned.at[job])
        wait_in(job, 2)
        attend(job)

    send_in(0, 0)
    send_in(0, 1)
    send_in(0, 2)
    send_in(1, 0, halves[0])
    clear_edges()
    for copy in weight_copies[:3]:
        copy.wait()
    for job in range(jobs):
        embed_bytes(job)
    for copy in weight_copies[3:]:
        copy.wait()
    turn_weights()
    attend_fore(0)
    send_in(1, 0, halves[1])
    send_in(1, 1)
    send_in(1, 2)
    for job in range(2, jobs):
        for n in range(3):
            send_in(job, n)
    byte_model(0)
    for job in range(1, jobs):
        attend_fore(job)
        attend_back(job - 1)
        byte_model(job)
        send_keys(job - 1, halves[1])
    send_losses()
    attend_back_last(jobs - 1)

    loss_others = losses.at[: grp_count - 1]
    pltpu.make_async_copy(loss_others, loss_others, loss_recv).wait()
    every = losses[0]
    for g in range(1, grp_count):
        every = every + losses[g]
    patches = lax.broadcasted_iota(jnp.int32, (rows, rows), 0)
    taken = (patches == order[...] - me_s * rows).astype(jnp.float32)
    by_slot = dot_exact(every, taken, ((0,), (0,)))[:PATCH]
    slots = lax.broadcasted_iota(jnp.int32, (rows, part), 0)
    mine = slots == lax.broadcasted_iota(jnp.int32, (rows, part), 1) + me_g * part
    loss_out[...] = dot_exact(by_slot, mine.astype(jnp.float32), ((1,), (0,)))

    pltpu.make_async_copy(loss_others, loss_others, loss_send).wait()
    sent = q_in.at[:, : (seq_count - 1) * jobs * HEAD]
    for n in range(3):
        pltpu.make_async_copy(sent, sent, in_send.at[n]).wait()
    others = ctx.at[:, :, : (seq_count - 1) * HEAD]
    pltpu.make_async_copy(others, others, ctx_send).wait()
    pltpu.make_async_copy(others, others, grad_send).wait()
    for n, target in enumerate((dq_out, dk_out, dv_out)):
        pltpu.make_async_copy(target, target, out_recv.at[n]).wait()
        pltpu.make_async_copy(sent, sent, out_send.at[n]).wait()


def fits(seq_count, grp_count, byte_ids, patch_order, query_rows, *rest):
    rows, columns = query_rows.shape
    vocab_size, model = rest[2].shape
    ffl = rest[4].shape[1]
    total = rows * seq_count
    return (
        PATCH % grp_count == 0
        and PATCH // grp_count >= 2
        and seq_count * HEAD == model
        and columns == PATCH // grp_count * model
        and rows % (16 * grp_count) == 0
        and rows // grp_count <= LANES
        and vocab_size % LANES == 0
        and total % KEY_TILE == 0
        and ffl % HIDDEN_TILE == 0
        and model % KEY_TILE == 0
        and PATCH // grp_count * total * total <= 6 * 1024 * 1024
    )


def fused_shards(
    seq_count,
    grp_count,
    byte_ids,
    patch_order,
    query_rows,
    key_rows,
    value_rows,
    byte_embed,
    norm_gain,
    w_up,
    w_down,
    vocab_head,
):
    rows, columns = query_rows.shape
    jobs = PATCH // grp_count
    total = rows * seq_count
    part = rows // grp_count
    vocab_size, model = byte_embed.shape
    ffl = w_up.shape[1]
    low, wide = jnp.bfloat16, jnp.float32
    anywhere = pl.BlockSpec(memory_space=pl.ANY)
    dma = pltpu.SemaphoreType.DMA
    by_job = [pltpu.VMEM((jobs, total, HEAD), low)] * 3
    losses, query_grad, key_grad, value_grad = pl.pallas_call(
        functools.partial(fused_kernel, seq_count, grp_count),
        out_shape=(pltpu.VMEM((PATCH, part), wide), *[pltpu.VMEM((rows, columns), low)] * 3),
        in_specs=[anywhere] * 10,
        out_specs=(pl.BlockSpec(memory_space=pltpu.VMEM), anywhere, anywhere, anywhere),
        scratch_shapes=[
            *by_job,
            pltpu.VMEM((jobs, total, total), low),
            pltpu.VMEM((jobs, total, HEAD), low),
            pltpu.VMEM((jobs, rows, model), low),
            pltpu.VMEM((jobs, rows, model), low),
            pltpu.VMEM((jobs, total, HEAD), low),
            *by_job,
            pltpu.VMEM((jobs, HEAD, total), low),
            pltpu.VMEM((HEAD, total), low),
            pltpu.VMEM((vocab_size, model), low),
            pltpu.VMEM((model, ffl), low),
            pltpu.VMEM((ffl, model), low),
            pltpu.VMEM((ffl, model), low),
            pltpu.VMEM((model, ffl), low),
            pltpu.VMEM((model, vocab_size), low),
            pltpu.VMEM((PATCH, rows), jnp.int32),
            pltpu.VMEM((1, rows), jnp.int32),
            pltpu.VMEM((1, model), wide),
            pltpu.VMEM((jobs, rows, model), wide),
            pltpu.VMEM((rows, model), low),
            pltpu.VMEM((rows, ffl), wide),
            pltpu.VMEM((rows, model), wide),
            pltpu.VMEM((rows, model), wide),
            pltpu.VMEM((rows, model), low),
            pltpu.VMEM((grp_count, rows, LANES), wide),
            dma((jobs, 3)),
            dma((3,)),
            dma((7,)),
            dma((jobs,)),
            dma,
            dma((jobs,)),
            dma,
            dma,
            dma,
            dma((3,)),
            dma((3,)),
        ],
        compiler_params=pltpu.CompilerParams(
            collective_id=0, has_side_effects=True, vmem_limit_bytes=64_000_000
        ),
    )(
        byte_ids.T,
        patch_order.reshape(1, rows),
        norm_gain.reshape(1, model),
        query_rows,
        key_rows,
        value_rows,
        byte_embed,
        w_up,
        w_down,
        vocab_head,
    )
    return losses.T, query_grad, key_grad, value_grad


def solution(mesh):
    placed = (
        P("seq", None),
        P("seq"),
        P("seq", "grp"),
        P("seq", "grp"),
        P("seq", "grp"),
        P(),
        P(),
        P(),
        P(),
        P(),
    )
    seq_count, grp_count = mesh.shape["seq"], mesh.shape["grp"]

    def body(*args):
        if fits(seq_count, grp_count, *args):
            return fused_shards(seq_count, grp_count, *args)
        return shards(*args)

    return jax.shard_map(
        body,
        mesh=mesh,
        in_specs=placed,
        out_specs=(P(("seq", "grp"), None), P("seq", "grp"), P("seq", "grp"), P("seq", "grp")),
        check_vma=False,
    )
```
